8 devices in a mesh: dp: 1 (over z), tp: 8 (over y, x, core).
Axes of the slice: x: 2, y: 2, z: 1, core: 2. Of those that a mesh axis runs over, the one named last changes fastest.
Arguments:
- query: bfloat16 [32, 32, 128], P('dp', 'tp')
- k_cache: bfloat16 [32, 1024, 32, 128], P('dp', None, 'tp')
- v_cache: bfloat16 [32, 1024, 32, 128], P('dp', None, 'tp')
- k_new: bfloat16 [32, 32, 128], P('dp', 'tp')
- v_new: bfloat16 [32, 32, 128], P('dp', 'tp')
- lens: int32 [32], P('dp')
Outputs:
- output 1: bfloat16 [32, 32, 128], P('dp', 'tp')
- output 2: bfloat16 [32, 1024, 32, 128], P('dp', 'tp')
- output 3: bfloat16 [32, 1024, 32, 128], P('dp', 'tp')
All inputs are finite; a program needn't handle non-finite values.
Results may differ from the reference program's by a relative error of at most 0.00763011.
Values are sent between devices in bfloat16 or wider.
A program may use at most 1 GiB of HBM per device.

```python
import math
import jax
import jax.numpy as jnp
from jax import lax

BATCH = 32
SEQ_LEN = 1024
Q_HEADS = 32
KV_HEADS = 32
HEAD_DIM = 128


def setup_inputs(seed: int = 0, part: int = 0) -> dict:
    base_key = jax.random.fold_in(jax.random.key(seed), part)
    keys = jax.random.split(base_key, 6)
    group_size = Q_HEADS // KV_HEADS
    spread = math.sqrt(math.log(SEQ_LEN))
    align = 1.4 * math.sqrt(math.log(SEQ_LEN) / HEAD_DIM)
    cache_shape = (BATCH, SEQ_LEN, KV_HEADS, HEAD_DIM)
    k_cache = jax.random.normal(keys[0], cache_shape, jnp.float32)
    v_cache = jax.random.normal(keys[1], cache_shape, jnp.float32)
    k_new = jax.random.normal(keys[2], (BATCH, KV_HEADS, HEAD_DIM), jnp.float32)
    v_new = jax.random.normal(keys[3], (BATCH, KV_HEADS, HEAD_DIM), jnp.float32)
    noise = jax.random.normal(keys[4], (BATCH, KV_HEADS, group_size, HEAD_DIM), jnp.float32)
    mixed = math.sqrt(1.0 - align * align) * noise + align * k_new[:, :, None, :]
    query = (spread * mixed).reshape(BATCH, Q_HEADS, HEAD_DIM)
    len_keys = jax.random.split(keys[5])
    low_len = SEQ_LEN // 8
    lens = jax.random.randint(len_keys[0], (BATCH,), low_len, SEQ_LEN, jnp.int32)
    top_slot = jax.random.randint(len_keys[1], (), 0, BATCH, jnp.int32)
    lens = jnp.where(jnp.arange(BATCH) == top_slot, SEQ_LEN - 1, lens)
    return {"query": query.astype(jnp.bfloat16), "k_cache": k_cache.astype(jnp.bfloat16), "v_cache": v_cache.astype(jnp.bfloat16), "k_new": k_new.astype(jnp.bfloat16), "v_new": v_new.astype(jnp.bfloat16), "lens": lens}


def reference(query, k_cache, v_cache, k_new, v_new, lens):
    positions = jnp.arange(SEQ_LEN, dtype=jnp.int32)
    new_slot = (positions[None, :] == lens[:, None])[:, :, None, None]
    k_upd = jnp.where(new_slot, k_new[:, None], k_cache)
    v_upd = jnp.where(new_slot, v_new[:, None], v_cache)
    group_size = Q_HEADS // KV_HEADS
    inv_sqrt = HEAD_DIM ** -0.5

    def one_head(head_in):
        q_head, k_head, v_head, length = head_in
        scores = jnp.dot(q_head, k_head.T, preferred_element_type=jnp.float32) * inv_sqrt
        scores = jnp.where(positions[None, :] <= length, scores, -1e30)
        probs = jax.nn.softmax(scores, axis=-1)
        return jnp.dot(probs.astype(jnp.bfloat16), v_head, preferred_element_type=jnp.float32)

    q_flat = query.reshape(BATCH * KV_HEADS, group_size, HEAD_DIM)
    k_flat = jnp.swapaxes(k_upd, 1, 2).reshape(BATCH * KV_HEADS, SEQ_LEN, HEAD_DIM)
    v_flat = jnp.swapaxes(v_upd, 1, 2).reshape(BATCH * KV_HEADS, SEQ_LEN, HEAD_DIM)
    len_flat = jnp.repeat(lens, KV_HEADS)
    head_out = lax.map(one_head, (q_flat, k_flat, v_flat, len_flat))
    attn_out = head_out.reshape(BATCH, Q_HEADS, HEAD_DIM).astype(jnp.bfloat16)
    return attn_out, k_upd, v_upd
```

```python
import functools

import jax
import jax.numpy as jnp
from jax import lax
from jax.experimental import pallas as pl
from jax.experimental.pallas import tpu as pltpu
from jax.sharding import PartitionSpec as P

RING = 4


def interleave_kernel(first, count, parts, extra, *refs):
    srcs = refs[:parts]
    out, buf, in_sem, out_sem = refs[parts + extra :]
    me = lax.axis_index("tp")
    ring = min(RING, count)

    def load(b, slot, k):
        return pltpu.make_async_copy(srcs[k].at[b], buf.at[slot, :, me ^ k], in_sem.at[slot, k])

    def store(b, slot):
        return pltpu.make_async_copy(buf.at[slot], out.at[first + b], out_sem.at[slot])

    for b in range(ring - 1 if count > ring else count):
        for k in range(parts):
            load(b, b, k).start()

    def step(b, carry):
        slot = lax.rem(b, ring)
        for k in range(parts):
            load(b, slot, k).wait()
        store(b, slot).start()
        if count > ring:
            ahead = b + ring - 1
            nxt = lax.rem(ahead, ring)

            @pl.when(ahead < count)
            def _():
                @pl.when(b > 0)
                def _():
                    store(b - 1, nxt).wait()

                for k in range(parts):
                    load(ahead, nxt, k).start()

        return carry

    lax.fori_loop(0, count, step, 0)
    for b in range(count - ring, count):
        store(b, b % ring).wait()


def interleave(pieces, first, batch, prev, after):
    parts, (count, seq, heads, dim) = len(pieces), pieces[0].shape
    args = tuple(pieces) + (() if prev is None else (prev,)) + tuple(after)
    moved = 2 * parts * pieces[0].size * 2
    return pl.pallas_call(
        functools.partial(interleave_kernel, first, count, parts, len(args) - parts),
        out_shape=jax.ShapeDtypeStruct((batch, seq, parts, heads, dim), pieces[0].dtype),
        in_specs=[pl.BlockSpec(memory_space=pl.ANY)] * len(args),
        out_specs=pl.BlockSpec(memory_space=pl.ANY),
        input_output_aliases={} if prev is None else {parts: 0},
        scratch_shapes=[
            pltpu.VMEM((min(RING, count), seq, parts, heads, dim), pieces[0].dtype),
            pltpu.SemaphoreType.DMA((min(RING, count), parts)),
            pltpu.SemaphoreType.DMA((min(RING, count),)),
        ],
        cost_estimate=pl.CostEstimate(flops=moved * 4, bytes_accessed=moved, transcendentals=0),
    )(*args)


def solution(mesh):
    tp = mesh.shape["tp"]

    def local_step(query, k_cache, v_cache, k_new, v_new, lens):
        batch, seq_len, heads, head_dim = k_cache.shape
        seq = seq_len // tp
        me = lax.axis_index("tp")
        group = query.shape[1] // heads

        def piece(cache, new, k, b0, b1):
            start = (me ^ k) * seq
            blk = lax.dynamic_slice(cache, (b0, start, 0, 0), (b1 - b0, seq, heads, head_dim))
            pos = start + lax.broadcasted_iota(jnp.int32, (1, seq, 1, 1), 1)
            return jnp.where(pos == lens[b0:b1, None, None, None], new[b0:b1, None], blk)

        def send(blk, k):
            if k == 0:
                return blk
            return lax.ppermute(blk, "tp", [(i, i ^ k) for i in range(tp)])

        order = [2, 4, 3, 5, 6, 7, 1, 0]
        head, tail = 4, 28
        caches, got = (k_cache, v_cache), {}

        def emit(which, ks, b0, b1):
            nonlocal caches
            new = (k_new, v_new)[which]
            blks = [piece(caches[which], new, k, b0, b1) for k in ks]
            caches, blks = lax.optimization_barrier((caches, blks))
            for k, blk in zip(ks, blks):
                got[which, b0, k] = send(blk, k)

        emit(0, [2, 4], 0, head)
        emit(0, [3, 5, 6, 7, 1, 0], 0, head)
        emit(0, order, head, batch)
        emit(1, order, 0, tail)
        emit(1, order, tail, batch)

        kc, vc = caches
        slot = lax.broadcasted_iota(jnp.int32, (1, seq_len, 1, 1), 1) == lens[:, None, None, None]
        k_upd = jnp.where(slot, k_new[:, None], kc)
        v_upd = jnp.where(slot, v_new[:, None], vc)
        q_grp = query.reshape(batch, heads, group, head_dim)
        scores = jnp.einsum("bhgd,bthd->bhgt", q_grp, k_upd, preferred_element_type=jnp.float32) * (head_dim ** -0.5)
        valid = lax.broadcasted_iota(jnp.int32, (1, 1, 1, seq_len), 3) <= lens[:, None, None, None]
        probs = jax.nn.softmax(jnp.where(valid, scores, -1e30), axis=-1)
        out = jnp.einsum("bhgt,bthd->bhgd", probs.astype(jnp.bfloat16), v_upd, preferred_element_type=jnp.float32)
        attn = out.reshape(batch, heads * group, head_dim).astype(jnp.bfloat16)

        def gather(which, b0, prev, after):
            return interleave([got[which, b0, k] for k in range(tp)], b0, batch, prev, after)

        k_out = gather(0, head, gather(0, 0, None, (attn,)), ())
        v_out = gather(1, tail, gather(1, 0, None, (k_out,)), ())
        shape = (batch, seq, tp * heads, head_dim)
        return attn, k_out.reshape(shape), v_out.reshape(shape)

    head_spec = P("dp", "tp")
    entry_spec = P("dp", None, "tp")
    return jax.shard_map(local_step, mesh=mesh, in_specs=(head_spec, entry_spec, entry_spec, head_spec, head_spec, P("dp")), out_specs=(head_spec, P("dp", "tp"), P("dp", "tp")), check_vma=False)
```

```python
import functools

import jax
import jax.numpy as jnp
from jax import lax
from jax.experimental import pallas as pl
from jax.experimental.pallas import tpu as pltpu
from jax.sharding import PartitionSpec as P

RING = 4
VMEM_BYTES = 67043328
ANY = pl.BlockSpec(memory_space=pl.ANY)


def ring_loop(count, load, work, store):
    ring = min(RING, count)

    def go(copies):
        for c in copies:
            c.start()

    def end(copies):
        for c in copies:
            c.wait()

    first = count if count == ring else ring - 1
    for i in range(first):
        go(load(i, i))

    def step(i, carry):
        slot = lax.rem(i, ring)
        end(load(i, slot))
        work(i, slot)
        go(store(i, slot))
        if first < count:
            ahead = i + first
            nxt = lax.rem(ahead, ring)

            @pl.when(ahead < count)
            def _():
                @pl.when(i > 0)
                def _():
                    end(store(i - 1, nxt))

                go(load(ahead, nxt))

        return carry

    lax.fori_loop(0, count, step, 0)
    for i in range(count - ring, count):
        end(store(i, i % ring))


def split_kernel(groups, outs, lens_ref, new_ref, cache_ref, *refs):
    out_refs = refs[-3 - len(outs) : -3]
    buf, in_sem, out_sem = refs[-3:]
    me = lax.axis_index("tp")
    seq = buf.shape[2]

    for b0, b1, ks in groups:
        dests = []
        for k in ks:
            i = next(i for i, (ok, lo, hi) in enumerate(outs) if ok == k and lo <= b0 and b1 <= hi)
            dests.append((out_refs[i], b0 - outs[i][1]))

        def load(i, slot):
            return [
                pltpu.make_async_copy(cache_ref.at[b0 + i, pl.ds((me ^ k) * seq, seq)], buf.at[slot, j], in_sem.at[slot, j])
                for j, k in enumerate(ks)
            ]

        def store(i, slot):
            return [
                pltpu.make_async_copy(buf.at[slot, j], ref.at[off + i], out_sem.at[slot, j])
                for j, (ref, off) in enumerate(dests)
            ]

        def work(i, slot):
            length = lens_ref[b0 + i]
            for j, k in enumerate(ks):
                row = length - (me ^ k) * seq

                @pl.when((row >= 0) & (row < seq))
                def _():
                    buf[slot, j, row] = new_ref[b0 + i]

        ring_loop(b1 - b0, load, work, store)


def split(cache, new, lens, groups, outs, seq, after):
    heads, dim = cache.shape[2:]
    width = max(len(ks) for _, _, ks in groups)
    moved = 2 * 2 * seq * heads * dim * sum((b1 - b0) * len(ks) for b0, b1, ks in groups)
    return pl.pallas_call(
        functools.partial(split_kernel, groups, outs),
        out_shape=[jax.ShapeDtypeStruct((hi - lo, seq, heads, dim), cache.dtype) for _, lo, hi in outs],
        in_specs=[pl.BlockSpec(memory_space=pltpu.SMEM), pl.BlockSpec(memory_space=pltpu.VMEM), ANY] + [ANY] * len(after),
        out_specs=[ANY] * len(outs),
        scratch_shapes=[
            pltpu.VMEM((RING, width, seq, heads, dim), cache.dtype),
            pltpu.SemaphoreType.DMA((RING, width)),
            pltpu.SemaphoreType.DMA((RING, width)),
        ],
        compiler_params=pltpu.CompilerParams(vmem_limit_bytes=VMEM_BYTES),
        cost_estimate=pl.CostEstimate(flops=moved * 4, bytes_accessed=moved, transcendentals=0),
    )(lens, new, cache, *after)


def join_kernel(segments, parts, used, *refs):
    srcs, out = refs[:used], refs[-4]
    buf, in_sem, out_sem = refs[-3:]
    me = lax.axis_index("tp")

    for b0, b1, where in segments:

        def load(i, slot):
            return [
                pltpu.make_async_copy(srcs[r].at[off + i], buf.at[slot, :, me ^ k], in_sem.at[slot, k])
                for k, (r, off) in enumerate(where)
            ]

        def store(i, slot):
            return [pltpu.make_async_copy(buf.at[slot], out.at[b0 + i], out_sem.at[slot])]

        ring_loop(b1 - b0, load, lambda i, slot: None, store)


def join(pieces, bounds, batch, parts, prev, after):
    keys = list(pieces)
    seq, heads, dim = pieces[keys[0]].shape[1:]
    segments = []
    for b0, b1 in zip(bounds[:-1], bounds[1:]):
        where = []
        for k in range(parts):
            key = next(key for key in keys if key[0] == k and key[1] <= b0 and b1 <= key[2])
            where.append((keys.index(key), b0 - key[1]))
        segments.append((b0, b1, where))
    args = [pieces[key] for key in keys] + ([] if prev is None else [prev]) + list(after)
    moved = 2 * 2 * seq * heads * dim * parts * (bounds[-1] - bounds[0])
    return pl.pallas_call(
        functools.partial(join_kernel, segments, parts, len(keys)),
        out_shape=jax.ShapeDtypeStruct((batch, seq, parts, heads, dim), pieces[keys[0]].dtype),
        in_specs=[ANY] * len(args),
        out_specs=ANY,
        input_output_aliases={} if prev is None else {len(keys): 0},
        scratch_shapes=[
            pltpu.VMEM((RING, seq, parts, heads, dim), pieces[keys[0]].dtype),
            pltpu.SemaphoreType.DMA((RING, parts)),
            pltpu.SemaphoreType.DMA((RING,)),
        ],
        compiler_params=pltpu.CompilerParams(vmem_limit_bytes=VMEM_BYTES),
        cost_estimate=pl.CostEstimate(flops=moved * 4, bytes_accessed=moved, transcendentals=0),
    )(*args)


def solution(mesh):
    tp = mesh.shape["tp"]

    def local_step(query, k_cache, v_cache, k_new, v_new, lens):
        batch, seq_len, heads, head_dim = k_cache.shape
        seq = seq_len // tp
        group = query.shape[1] // heads

        def send(arr, k):
            return arr if k == 0 else lax.ppermute(arr, "tp", [(i, i ^ k) for i in range(tp)])

        lead = [k for k in (2, 4) if k < tp]
        rest = [k for k in (3, 5, 6, 7, 1, 0) if k < tp]
        order = lead + rest
        c1, c2 = batch // 8, batch // 2
        v1, v2 = batch - batch // 4, batch - batch // 16
        got = ({}, {})

        def emit(which, groups, outs, after):
            cache, new = ((k_cache, k_new), (v_cache, v_new))[which]
            arrs = split(cache, new, lens, groups, outs, seq, after)
            for key, arr in zip(outs, arrs):
                got[which][key] = send(arr, key[0])
            return [arrs[-1]]

        tok = emit(0, [(0, c1, lead)], [(k, 0, c1) for k in lead], [])
        tok = emit(0, [(c1, c2, lead)], [(k, c1, c2) for k in lead], tok)
        tok = emit(0, [(c2, batch, order), (0, c2, rest)], [(k, c2, batch) for k in lead] + [(k, 0, batch) for k in rest], tok)
        vb = [0, v1, v2, batch]
        for lo, hi in zip(vb[:-1], vb[1:]):
            tok = emit(1, [(lo, hi, order)], [(k, lo, hi) for k in order], tok)

        kc, vc, _ = lax.optimization_barrier((k_cache, v_cache, tok))
        slot = lax.broadcasted_iota(jnp.int32, (1, seq_len, 1, 1), 1) == lens[:, None, None, None]
        k_upd = jnp.where(slot, k_new[:, None], kc)
        v_upd = jnp.where(slot, v_new[:, None], vc)
        q_grp = query.reshape(batch, heads, group, head_dim)
        scores = jnp.einsum("bhgd,bthd->bhgt", q_grp, k_upd, preferred_element_type=jnp.float32) * (head_dim ** -0.5)
        valid = lax.broadcasted_iota(jnp.int32, (1, 1, 1, seq_len), 3) <= lens[:, None, None, None]
        probs = jax.nn.softmax(jnp.where(valid, scores, -1e30), axis=-1)
        out = jnp.einsum("bhgt,bthd->bhgd", probs.astype(jnp.bfloat16), v_upd, preferred_element_type=jnp.float32)
        attn = out.reshape(batch, heads * group, head_dim).astype(jnp.bfloat16)

        k_out = join(got[0], [0, c1, c2, batch], batch, tp, None, [attn])
        v_out, after = None, [k_out]
        for lo, hi in zip(vb[:-1], vb[1:]):
            part = {key: arr for key, arr in got[1].items() if key[1] == lo}
            v_out = join(part, [lo, hi], batch, tp, v_out, after)
            after = []
        shape = (batch, seq, tp * heads, head_dim)
        return attn, k_out.reshape(shape), v_out.reshape(shape)

    head_spec = P("dp", "tp")
    entry_spec = P("dp", None, "tp")
    return jax.shard_map(local_step, mesh=mesh, in_specs=(head_spec, entry_spec, entry_spec, head_spec, head_spec, P("dp")), out_specs=(head_spec, P("dp", "tp"), P("dp", "tp")), check_vma=False)
```

```python
import functools

import jax
import jax.numpy as jnp
from jax import lax
from jax.experimental import pallas as pl
from jax.experimental.pallas import tpu as pltpu
from jax.sharding import PartitionSpec as P

RING = 4
VMEM_BYTES = 67043328
SMALL_BYTES = 24 << 20
ANY = pl.BlockSpec(memory_space=pl.ANY)


def ring_loop(count, load, loaded, work, store, ready=()):
    ring = min(RING, count)

    def go(copies):
        for c in copies:
            c.start()

    def end(copies):
        for c in copies:
            c.wait()

    first = count if count == ring else ring - 1
    for i in range(first):
        go(load(i, i))
    end(ready)

    def step(i, carry):
        slot = lax.rem(i, ring)
        end(loaded(i, slot))
        work(i, slot)
        go(store(i, slot))
        if first < count:
            ahead = i + first
            nxt = lax.rem(ahead, ring)

            @pl.when(ahead < count)
            def _():
                @pl.when(i > 0)
                def _():
                    end(store(i - 1, nxt))

                go(load(ahead, nxt))

        return carry

    lax.fori_loop(0, count, step, 0)
    for i in range(count - ring, count):
        end(store(i, i % ring))


def per_step(count):
    return next(n for n in (4, 2, 1) if count % n == 0)


def split_kernel(groups, outs, lens_hbm, new_hbm, cache_ref, *refs):
    out_refs = refs[-6 - len(outs) : -6]
    buf, lens_ref, new_ref, in_sem, out_sem, small_sem = refs[-6:]
    ready = [
        pltpu.make_async_copy(lens_hbm, lens_ref, small_sem.at[0]),
        pltpu.make_async_copy(new_hbm, new_ref, small_sem.at[1]),
    ]
    for c in ready:
        c.start()
    me = lax.axis_index("tp")
    seq_len = buf.shape[2]
    seq = seq_len // lax.axis_size("tp")

    for b0, b1, ks, n in groups:
        dests = []
        for k in ks:
            i = next(i for i, (ok, lo, hi) in enumerate(outs) if ok == k and lo <= b0 and b1 <= hi)
            dests.append((out_refs[i], b0 - outs[i][1]))

        def load(i, slot):
            rows = pl.ds(b0 + i * n, n)
            if 2 * len(ks) > lax.axis_size("tp"):
                return [pltpu.make_async_copy(cache_ref.at[rows], buf.at[slot, pl.ds(0, n)], in_sem.at[slot, 0])]
            return [
                pltpu.make_async_copy(
                    cache_ref.at[rows, pl.ds((me ^ k) * seq, seq)],
                    buf.at[slot, pl.ds(0, n), pl.ds((me ^ k) * seq, seq)],
                    in_sem.at[slot, j],
                )
                for j, k in enumerate(ks)
            ]

        def store(i, slot):
            return [
                pltpu.make_async_copy(
                    buf.at[slot, pl.ds(0, n), pl.ds((me ^ k) * seq, seq)], ref.at[pl.ds(off + i * n, n)], out_sem.at[slot, j]
                )
                for j, (k, (ref, off)) in enumerate(zip(ks, dests))
            ]

        def work(i, slot):
            for r in range(n):
                b = b0 + i * n + r
                buf[slot, r, lens_ref[b]] = new_ref[b]

        ring_loop((b1 - b0) // n, load, load, work, store, ready)
        ready = []


def split(cache, new, lens, groups, outs, parts, after):
    seq_len, heads, dim = cache.shape[1:]
    seq = seq_len // parts
    moved = 2 * 2 * seq * heads * dim * sum((b1 - b0) * len(ks) for b0, b1, ks, _ in groups)
    return pl.pallas_call(
        functools.partial(split_kernel, groups, outs),
        out_shape=[jax.ShapeDtypeStruct((hi - lo, seq, heads, dim), cache.dtype) for _, lo, hi in outs],
        in_specs=[ANY] * (3 + len(after)),
        out_specs=[ANY] * len(outs),
        scratch_shapes=[
            pltpu.VMEM((RING, max(n for _, _, _, n in groups), seq_len, heads, dim), cache.dtype),
            pltpu.SMEM(lens.shape, lens.dtype),
            pltpu.VMEM(new.shape, new.dtype),
            pltpu.SemaphoreType.DMA((RING, parts)),
            pltpu.SemaphoreType.DMA((RING, parts)),
            pltpu.SemaphoreType.DMA((2,)),
        ],
        compiler_params=pltpu.CompilerParams(vmem_limit_bytes=VMEM_BYTES),
        cost_estimate=pl.CostEstimate(flops=moved * 4, bytes_accessed=moved, transcendentals=0),
    )(lens, new, cache, *after)


def join_kernel(segments, parts, used, *refs):
    srcs, out = refs[:used], refs[-4]
    buf, in_sem, out_sem = refs[-3:]
    me = lax.axis_index("tp")

    for b0, b1, where in segments:
        n = per_step(b1 - b0)

        def load(i, slot):
            return [
                pltpu.make_async_copy(srcs[r].at[pl.ds(off + i * n, n)], buf.at[slot, pl.ds(0, n), :, me ^ k], in_sem.at[slot])
                for k, (r, off) in enumerate(where)
            ]

        def loaded(i, slot):
            return [pltpu.make_async_copy(out.at[pl.ds(b0, n)], buf.at[slot, pl.ds(0, n)], in_sem.at[slot])]

        def store(i, slot):
            return [pltpu.make_async_copy(buf.at[slot, pl.ds(0, n)], out.at[pl.ds(b0 + i * n, n)], out_sem.at[slot])]

        ring_loop((b1 - b0) // n, load, loaded, lambda i, slot: None, store)


def join(pieces, bounds, batch, parts, prev, after, limit):
    keys = list(pieces)
    seq, heads, dim = pieces[keys[0]].shape[1:]
    segments = []
    for b0, b1 in zip(bounds[:-1], bounds[1:]):
        where = []
        for k in range(parts):
            key = next(key for key in keys if key[0] == k and key[1] <= b0 and b1 <= key[2])
            where.append((keys.index(key), b0 - key[1]))
        segments.append((b0, b1, where))
    args = [pieces[key] for key in keys] + ([] if prev is None else [prev]) + list(after)
    moved = 2 * 2 * seq * heads * dim * parts * (bounds[-1] - bounds[0])
    return pl.pallas_call(
        functools.partial(join_kernel, segments, parts, len(keys)),
        out_shape=jax.ShapeDtypeStruct((batch, seq, parts, heads, dim), pieces[keys[0]].dtype),
        in_specs=[ANY] * len(args),
        out_specs=ANY,
        input_output_aliases={} if prev is None else {len(keys): 0},
        scratch_shapes=[
            pltpu.VMEM((RING, max(per_step(b1 - b0) for b0, b1, _ in segments), seq, parts, heads, dim), pieces[keys[0]].dtype),
            pltpu.SemaphoreType.DMA((RING,)),
            pltpu.SemaphoreType.DMA((RING,)),
        ],
        compiler_params=pltpu.CompilerParams(vmem_limit_bytes=limit),
        cost_estimate=pl.CostEstimate(flops=moved * 4, bytes_accessed=moved, transcendentals=0),
    )(*args)


def last_join_kernel(b0, parts, *refs):
    srcs, out, sem = refs[:parts], refs[-2], refs[-1]
    me = lax.axis_index("tp")
    copies = [pltpu.make_async_copy(srcs[k], out.at[pl.ds(b0, srcs[k].shape[0]), :, me ^ k], sem.at[k]) for k in range(parts)]
    for c in copies:
        c.start()
    for c in copies:
        c.wait()


def last_join(pieces, b0, prev):
    parts = len(pieces)
    return pl.pallas_call(
        functools.partial(last_join_kernel, b0, parts),
        out_shape=jax.ShapeDtypeStruct(prev.shape, prev.dtype),
        in_specs=[pl.BlockSpec(memory_space=pltpu.VMEM)] * parts + [ANY],
        out_specs=ANY,
        input_output_aliases={parts: 0},
        scratch_shapes=[pltpu.SemaphoreType.DMA((parts,))],
        compiler_params=pltpu.CompilerParams(vmem_limit_bytes=SMALL_BYTES),
        cost_estimate=pl.CostEstimate(flops=1 << 20, bytes_accessed=1 << 20, transcendentals=0),
    )(*pieces, prev)


def solution(mesh):
    tp = mesh.shape["tp"]

    def local_step(query, k_cache, v_cache, k_new, v_new, lens):
        batch, seq_len, heads, head_dim = k_cache.shape
        seq = seq_len // tp
        group = query.shape[1] // heads

        def send(arr, k):
            return arr if k == 0 else lax.ppermute(arr, "tp", [(i, i ^ k) for i in range(tp)])

        lead = [k for k in (2, 4) if k < tp]
        rest = [k for k in (3, 5, 6, 7, 1, 0) if k < tp]
        order = lead + rest
        c1, c2 = batch // 8, batch // 2
        v1, v2 = batch - batch // 4, batch - 1
        got = ({}, {})

        def emit(which, groups, outs, after):
            cache, new = ((k_cache, k_new), (v_cache, v_new))[which]
            arrs = split(cache, new, lens, groups, outs, tp, after)
            for key, arr in zip(outs, arrs):
                got[which][key] = send(arr, key[0])
            return [arrs[-1]]

        tok = emit(0, [(0, c1, lead, 1)], [(k, 0, c1) for k in lead], [])
        tok = emit(0, [(c1, c2, lead, per_step(c2 - c1))], [(k, c1, c2) for k in lead], tok)
        tok = emit(0, [(c2, batch, order, per_step(batch - c2)), (0, c2, rest, per_step(c2))],
                   [(k, c2, batch) for k in lead] + [(k, 0, batch) for k in rest], tok)
        vb = [0, v1, v2, batch]
        for lo, hi in zip(vb[:-2], vb[1:-1]):
            tok = emit(1, [(lo, hi, order, per_step(hi - lo))], [(k, lo, hi) for k in order], tok)

        kc, vc, _ = lax.optimization_barrier((k_cache, v_cache, tok))
        slot = lax.broadcasted_iota(jnp.int32, (1, seq_len, 1, 1), 1) == lens[:, None, None, None]
        k_upd = jnp.where(slot, k_new[:, None], kc)
        v_upd = jnp.where(slot, v_new[:, None], vc)
        q_grp = query.reshape(batch, heads, group, head_dim)
        scores = jnp.einsum("bhgd,bthd->bhgt", q_grp, k_upd, preferred_element_type=jnp.float32) * (head_dim ** -0.5)
        valid = lax.broadcasted_iota(jnp.int32, (1, 1, 1, seq_len), 3) <= lens[:, None, None, None]
        probs = jax.nn.softmax(jnp.where(valid, scores, -1e30), axis=-1)
        out = jnp.einsum("bhgt,bthd->bhgd", probs.astype(jnp.bfloat16), v_upd, preferred_element_type=jnp.float32)
        attn = out.reshape(batch, heads * group, head_dim).astype(jnp.bfloat16)

        k_out = join(got[0], [0, c1, c2, batch], batch, tp, None, [attn], VMEM_BYTES)
        emit(1, [(v2, batch, order, 1)], [(k, v2, batch) for k in order], [k_out])
        v_out, after = None, [k_out]
        for lo, hi in zip(vb[:-2], vb[1:-1]):
            part = {key: arr for key, arr in got[1].items() if key[1] == lo}
            v_out = join(part, [lo, hi], batch, tp, v_out, after, SMALL_BYTES)
            after = []
        v_out = last_join([got[1][k, v2, batch] for k in range(tp)], v2, v_out)
        shape = (batch, seq, tp * heads, head_dim)
        return attn, k_out.reshape(shape), v_out.reshape(shape)

    head_spec = P("dp", "tp")
    entry_spec = P("dp", None, "tp")
    return jax.shard_map(local_step, mesh=mesh, in_specs=(head_spec, entry_spec, entry_spec, head_spec, head_spec, P("dp")), out_specs=(head_spec, P("dp", "tp"), P("dp", "tp")), check_vma=False)
```

```python
import functools

import jax
import jax.numpy as jnp
from jax import lax
from jax.experimental import pallas as pl
from jax.experimental.pallas import tpu as pltpu
from jax.sharding import PartitionSpec as P

RING = 4
VMEM_BYTES = 67043328
MOST_BYTES = VMEM_BYTES - (3 << 20)
SMALL_BYTES = 24 << 20
ANY = pl.BlockSpec(memory_space=pl.ANY)


def ring_loop(count, load, loaded, work, store, ready=()):
    ring = min(RING, count)

    def go(copies):
        for c in copies:
            c.start()

    def end(copies):
        for c in copies:
            c.wait()

    first = count if count == ring else ring - 1
    for i in range(first):
        go(load(i, i))
    end(ready)

    def step(i, carry):
        slot = lax.rem(i, ring)
        end(loaded(i, slot))
        work(i, slot)
        go(store(i, slot))
        if first < count:
            ahead = i + first
            nxt = lax.rem(ahead, ring)

            @pl.when(ahead < count)
            def _():
                @pl.when(i > 0)
                def _():
                    end(store(i - 1, nxt))

                go(load(ahead, nxt))

        return carry

    lax.fori_loop(0, count, step, 0)
    for i in range(count - ring, count):
        end(store(i, i % ring))


def per_step(count):
    return next(n for n in (4, 2, 1) if count % n == 0)


def split_kernel(groups, outs, lens_hbm, new_hbm, cache_ref, *refs):
    out_refs = refs[-6 - len(outs) : -6]
    buf, lens_ref, new_ref, in_sem, out_sem, small_sem = refs[-6:]
    ready = [
        pltpu.make_async_copy(lens_hbm, lens_ref, small_sem.at[0]),
        pltpu.make_async_copy(new_hbm, new_ref, small_sem.at[1]),
    ]
    for c in ready:
        c.start()
    me = lax.axis_index("tp")
    seq_len = buf.shape[2]
    seq = seq_len // lax.axis_size("tp")

    for b0, b1, ks, n in groups:
        dests = []
        for k in ks:
            i = next(i for i, (ok, lo, hi) in enumerate(outs) if ok == k and lo <= b0 and b1 <= hi)
            dests.append((out_refs[i], b0 - outs[i][1]))

        def load(i, slot):
            rows = pl.ds(b0 + i * n, n)
            if 2 * len(ks) > lax.axis_size("tp"):
                return [pltpu.make_async_copy(cache_ref.at[rows], buf.at[slot, pl.ds(0, n)], in_sem.at[slot, 0])]
            return [
                pltpu.make_async_copy(
                    cache_ref.at[rows, pl.ds((me ^ k) * seq, seq)],
                    buf.at[slot, pl.ds(0, n), pl.ds((me ^ k) * seq, seq)],
                    in_sem.at[slot, j],
                )
                for j, k in enumerate(ks)
            ]

        def store(i, slot):
            return [
                pltpu.make_async_copy(
                    buf.at[slot, pl.ds(0, n), pl.ds((me ^ k) * seq, seq)], ref.at[pl.ds(off + i * n, n)], out_sem.at[slot, j]
                )
                for j, (k, (ref, off)) in enumerate(zip(ks, dests))
            ]

        def work(i, slot):
            for r in range(n):
                b = b0 + i * n + r
                buf[slot, r, lens_ref[b]] = new_ref[b]

        ring_loop((b1 - b0) // n, load, load, work, store, ready)
        ready = []


def split(cache, new, lens, groups, outs, parts, after, limit):
    seq_len, heads, dim = cache.shape[1:]
    seq = seq_len // parts
    moved = 2 * 2 * seq * heads * dim * sum((b1 - b0) * len(ks) for b0, b1, ks, _ in groups)
    return pl.pallas_call(
        functools.partial(split_kernel, groups, outs),
        out_shape=[jax.ShapeDtypeStruct((hi - lo, seq, heads, dim), cache.dtype) for _, lo, hi in outs],
        in_specs=[ANY] * (3 + len(after)),
        out_specs=[ANY] * len(outs),
        scratch_shapes=[
            pltpu.VMEM((RING, max(n for _, _, _, n in groups), seq_len, heads, dim), cache.dtype),
            pltpu.SMEM(lens.shape, lens.dtype),
            pltpu.VMEM(new.shape, new.dtype),
            pltpu.SemaphoreType.DMA((RING, parts)),
            pltpu.SemaphoreType.DMA((RING, parts)),
            pltpu.SemaphoreType.DMA((2,)),
        ],
        compiler_params=pltpu.CompilerParams(vmem_limit_bytes=limit),
        cost_estimate=pl.CostEstimate(flops=moved * 4, bytes_accessed=moved, transcendentals=0),
    )(lens, new, cache, *after)


def first_split_kernel(ks, lens_hbm, new_hbm, cache_ref, *refs):
    out_refs = refs[: len(ks)]
    lens_ref, new_ref, sem = refs[len(ks) :]
    me = lax.axis_index("tp")
    count, seq = out_refs[0].shape[:2]
    copies = [pltpu.make_async_copy(lens_hbm, lens_ref, sem.at[0]), pltpu.make_async_copy(new_hbm.at[pl.ds(0, count)], new_ref, sem.at[1])]
    for j, k in enumerate(ks):
        copies.append(pltpu.make_async_copy(cache_ref.at[pl.ds(0, count), pl.ds((me ^ k) * seq, seq)], out_refs[j], sem.at[2 + j]))
    for c in copies:
        c.start()
    for c in copies:
        c.wait()
    for b in range(count):
        length = lens_ref[b]
        for j, k in enumerate(ks):
            row = length - (me ^ k) * seq

            @pl.when((row >= 0) & (row < seq))
            def _():
                out_refs[j][b, row] = new_ref[b]


def first_split(cache, new, lens, count, ks, parts):
    seq_len, heads, dim = cache.shape[1:]
    seq = seq_len // parts
    return pl.pallas_call(
        functools.partial(first_split_kernel, ks),
        out_shape=[pltpu.VMEM((count, seq, heads, dim), cache.dtype) for _ in ks],
        in_specs=[ANY] * 3,
        out_specs=[pl.BlockSpec(memory_space=pltpu.VMEM)] * len(ks),
        scratch_shapes=[
            pltpu.SMEM(lens.shape, lens.dtype),
            pltpu.VMEM((count,) + new.shape[1:], new.dtype),
            pltpu.SemaphoreType.DMA((2 + len(ks),)),
        ],
        compiler_params=pltpu.CompilerParams(vmem_limit_bytes=MOST_BYTES),
        cost_estimate=pl.CostEstimate(flops=1 << 20, bytes_accessed=1 << 20, transcendentals=0),
    )(lens, new, cache)


def join_kernel(segments, parts, used, *refs):
    srcs, out = refs[:used], refs[-4]
    buf, in_sem, out_sem = refs[-3:]
    me = lax.axis_index("tp")

    for b0, b1, where in segments:
        n = per_step(b1 - b0)

        def load(i, slot):
            return [
                pltpu.make_async_copy(srcs[r].at[pl.ds(off + i * n, n)], buf.at[slot, pl.ds(0, n), :, me ^ k], in_sem.at[slot])
                for k, (r, off) in enumerate(where)
            ]

        def loaded(i, slot):
            return [pltpu.make_async_copy(out.at[pl.ds(b0, n)], buf.at[slot, pl.ds(0, n)], in_sem.at[slot])]

        def store(i, slot):
            return [pltpu.make_async_copy(buf.at[slot, pl.ds(0, n)], out.at[pl.ds(b0 + i * n, n)], out_sem.at[slot])]

        ring_loop((b1 - b0) // n, load, loaded, lambda i, slot: None, store)


def join(pieces, bounds, batch, parts, prev, after, limit):
    keys = list(pieces)
    seq, heads, dim = pieces[keys[0]].shape[1:]
    segments = []
    for b0, b1 in zip(bounds[:-1], bounds[1:]):
        where = []
        for k in range(parts):
            key = next(key for key in keys if key[0] == k and key[1] <= b0 and b1 <= key[2])
            where.append((keys.index(key), b0 - key[1]))
        segments.append((b0, b1, where))
    args = [pieces[key] for key in keys] + ([] if prev is None else [prev]) + list(after)
    moved = 2 * 2 * seq * heads * dim * parts * (bounds[-1] - bounds[0])
    return pl.pallas_call(
        functools.partial(join_kernel, segments, parts, len(keys)),
        out_shape=jax.ShapeDtypeStruct((batch, seq, parts, heads, dim), pieces[keys[0]].dtype),
        in_specs=[ANY] * len(args),
        out_specs=ANY,
        input_output_aliases={} if prev is None else {len(keys): 0},
        scratch_shapes=[
            pltpu.VMEM((RING, max(per_step(b1 - b0) for b0, b1, _ in segments), seq, parts, heads, dim), pieces[keys[0]].dtype),
            pltpu.SemaphoreType.DMA((RING,)),
            pltpu.SemaphoreType.DMA((RING,)),
        ],
        compiler_params=pltpu.CompilerParams(vmem_limit_bytes=limit),
        cost_estimate=pl.CostEstimate(flops=moved * 4, bytes_accessed=moved, transcendentals=0),
    )(*args)


def last_join_kernel(b0, parts, *refs):
    srcs, out, sem = refs[:parts], refs[-2], refs[-1]
    me = lax.axis_index("tp")
    copies = [pltpu.make_async_copy(srcs[k], out.at[pl.ds(b0, srcs[k].shape[0]), :, me ^ k], sem.at[k]) for k in range(parts)]
    for c in copies:
        c.start()
    for c in copies:
        c.wait()


def last_join(pieces, b0, prev):
    parts = len(pieces)
    return pl.pallas_call(
        functools.partial(last_join_kernel, b0, parts),
        out_shape=jax.ShapeDtypeStruct(prev.shape, prev.dtype),
        in_specs=[pl.BlockSpec(memory_space=pltpu.VMEM)] * parts + [ANY],
        out_specs=ANY,
        input_output_aliases={parts: 0},
        scratch_shapes=[pltpu.SemaphoreType.DMA((parts,))],
        compiler_params=pltpu.CompilerParams(vmem_limit_bytes=SMALL_BYTES),
        cost_estimate=pl.CostEstimate(flops=1 << 20, bytes_accessed=1 << 20, transcendentals=0),
    )(*pieces, prev)


def solution(mesh):
    tp = mesh.shape["tp"]

    def local_step(query, k_cache, v_cache, k_new, v_new, lens):
        batch, seq_len, heads, head_dim = k_cache.shape
        seq = seq_len // tp
        group = query.shape[1] // heads

        def send(arr, k):
            return arr if k == 0 else lax.ppermute(arr, "tp", [(i, i ^ k) for i in range(tp)])

        lead = [k for k in (2, 4) if k < tp]
        rest = [k for k in (3, 5, 6, 7, 1, 0) if k < tp]
        order = lead + rest
        c1, c2 = batch // 8, batch // 2
        v1, v2 = batch - batch // 4, batch - 1
        got = ({}, {})

        def emit(which, groups, outs, after):
            cache, new = ((k_cache, k_new), (v_cache, v_new))[which]
            arrs = split(cache, new, lens, groups, outs, tp, after, MOST_BYTES)
            for key, arr in zip(outs, arrs):
                got[which][key] = send(arr, key[0])
            return [arrs[-1]]

        tok = first_split(k_cache, k_new, lens, c1, lead, tp)
        for k, arr in zip(lead, tok):
            got[0][k, 0, c1] = send(arr, k)
        tok = emit(0, [(c1, c2, lead, per_step(c2 - c1))], [(k, c1, c2) for k in lead], [])
        tok = emit(0, [(c2, batch, order, per_step(batch - c2)), (0, c2, rest, per_step(c2))],
                   [(k, c2, batch) for k in lead] + [(k, 0, batch) for k in rest], tok)
        vb = [0, v1, v2, batch]
        tok = emit(1, [(0, v1, order, per_step(v1))], [(k, 0, v1) for k in order], tok)

        kc, vc, _ = lax.optimization_barrier((k_cache, v_cache, tok))
        slot = lax.broadcasted_iota(jnp.int32, (1, seq_len, 1, 1), 1) == lens[:, None, None, None]
        k_upd = jnp.where(slot, k_new[:, None], kc)
        v_upd = jnp.where(slot, v_new[:, None], vc)
        q_grp = query.reshape(batch, heads, group, head_dim)
        scores = jnp.einsum("bhgd,bthd->bhgt", q_grp, k_upd, preferred_element_type=jnp.float32) * (head_dim ** -0.5)
        valid = lax.broadcasted_iota(jnp.int32, (1, 1, 1, seq_len), 3) <= lens[:, None, None, None]
        probs = jax.nn.softmax(jnp.where(valid, scores, -1e30), axis=-1)
        out = jnp.einsum("bhgt,bthd->bhgd", probs.astype(jnp.bfloat16), v_upd, preferred_element_type=jnp.float32)
        attn = out.reshape(batch, heads * group, head_dim).astype(jnp.bfloat16)

        k_out = join(got[0], [0, c1, c2, batch], batch, tp, None, [attn], MOST_BYTES)
        tok = emit(1, [(v1, v2, order, per_step(v2 - v1))], [(k, v1, v2) for k in order], [k_out])
        emit(1, [(v2, batch, order, 1)], [(k, v2, batch) for k in order], tok)
        v_out, after = None, [k_out]
        for lo, hi in zip(vb[:-2], vb[1:-1]):
            part = {key: arr for key, arr in got[1].items() if key[1] == lo}
            v_out = join(part, [lo, hi], batch, tp, v_out, after, SMALL_BYTES)
            after = []
        v_out = last_join([got[1][k, v2, batch] for k in range(tp)], v2, v_out)
        shape = (batch, seq, tp * heads, head_dim)
        return attn, k_out.reshape(shape), v_out.reshape(shape)

    head_spec = P("dp", "tp")
    entry_spec = P("dp", None, "tp")
    return jax.shard_map(local_step, mesh=mesh, in_specs=(head_spec, entry_spec, entry_spec, head_spec, head_spec, P("dp")), out_specs=(head_spec, P("dp", "tp"), P("dp", "tp")), check_vma=False)
```

```python
import functools

import jax
import jax.numpy as jnp
from jax import lax
from jax.experimental import pallas as pl
from jax.experimental.pallas import tpu as pltpu
from jax.sharding import PartitionSpec as P

RING = 4
VMEM_BYTES = 67043328
MOST_BYTES = VMEM_BYTES - (3 << 20)
SMALL_BYTES = 40 << 20
ANY = pl.BlockSpec(memory_space=pl.ANY)


def ring_loop(count, load, loaded, work, store, ready=()):
    ring = min(RING, count)

    def go(copies):
        for c in copies:
            c.start()

    def end(copies):
        for c in copies:
            c.wait()

    first = count if count == ring else ring - 1
    for i in range(first):
        go(load(i, i))
    end(ready)

    def step(i, carry):
        slot = lax.rem(i, ring)
        end(loaded(i, slot))
        work(i, slot)
        go(store(i, slot))
        if first < count:
            ahead = i + first
            nxt = lax.rem(ahead, ring)

            @pl.when(ahead < count)
            def _():
                @pl.when(i > 0)
                def _():
                    end(store(i - 1, nxt))

                go(load(ahead, nxt))

        return carry

    lax.fori_loop(0, count, step, 0)
    for i in range(count - ring, count):
        end(store(i, i % ring))


def per_step(count):
    return next(n for n in range(8, 0, -1) if count % n == 0)


def split_kernel(groups, outs, lens_hbm, new_hbm, cache_ref, *refs):
    out_refs = refs[-6 - len(outs) : -6]
    buf, lens_ref, new_ref, in_sem, out_sem, small_sem = refs[-6:]
    ready = [
        pltpu.make_async_copy(lens_hbm, lens_ref, small_sem.at[0]),
        pltpu.make_async_copy(new_hbm, new_ref, small_sem.at[1]),
    ]
    for c in ready:
        c.start()
    me = lax.axis_index("tp")
    seq_len = buf.shape[2]
    seq = seq_len // lax.axis_size("tp")

    for b0, b1, ks, n in groups:
        dests = []
        for k in ks:
            i = next(i for i, (ok, lo, hi) in enumerate(outs) if ok == k and lo <= b0 and b1 <= hi)
            dests.append((out_refs[i], b0 - outs[i][1]))

        def load(i, slot):
            rows = pl.ds(b0 + i * n, n)
            if 2 * len(ks) > lax.axis_size("tp"):
                return [pltpu.make_async_copy(cache_ref.at[rows], buf.at[slot, pl.ds(0, n)], in_sem.at[slot, 0])]
            return [
                pltpu.make_async_copy(
                    cache_ref.at[rows, pl.ds((me ^ k) * seq, seq)],
                    buf.at[slot, pl.ds(0, n), pl.ds((me ^ k) * seq, seq)],
                    in_sem.at[slot, j],
                )
                for j, k in enumerate(ks)
            ]

        def store(i, slot):
            return [
                pltpu.make_async_copy(
                    buf.at[slot, pl.ds(0, n), pl.ds((me ^ k) * seq, seq)], ref.at[pl.ds(off + i * n, n)], out_sem.at[slot, j]
                )
                for j, (k, (ref, off)) in enumerate(zip(ks, dests))
            ]

        def work(i, slot):
            for r in range(n):
                b = b0 + i * n + r
                buf[slot, r, lens_ref[b]] = new_ref[b]

        ring_loop((b1 - b0) // n, load, load, work, store, ready)
        ready = []


def split(cache, new, lens, groups, outs, parts, after, limit):
    seq_len, heads, dim = cache.shape[1:]
    seq = seq_len // parts
    moved = 2 * 2 * seq * heads * dim * sum((b1 - b0) * len(ks) for b0, b1, ks, _ in groups)
    return pl.pallas_call(
        functools.partial(split_kernel, groups, outs),
        out_shape=[jax.ShapeDtypeStruct((hi - lo, seq, heads, dim), cache.dtype) for _, lo, hi in outs],
        in_specs=[ANY] * (3 + len(after)),
        out_specs=[ANY] * len(outs),
        scratch_shapes=[
            pltpu.VMEM((RING, max(n for _, _, _, n in groups), seq_len, heads, dim), cache.dtype),
            pltpu.SMEM(lens.shape, lens.dtype),
            pltpu.VMEM(new.shape, new.dtype),
            pltpu.SemaphoreType.DMA((RING, parts)),
            pltpu.SemaphoreType.DMA((RING, parts)),
            pltpu.SemaphoreType.DMA((2,)),
        ],
        compiler_params=pltpu.CompilerParams(vmem_limit_bytes=limit),
        cost_estimate=pl.CostEstimate(flops=moved * 4, bytes_accessed=moved, transcendentals=0),
    )(lens, new, cache, *after)


def first_split_kernel(ks, lens_hbm, new_hbm, cache_ref, *refs):
    out_refs = refs[: len(ks)]
    lens_ref, new_ref, sem = refs[len(ks) :]
    me = lax.axis_index("tp")
    count, seq = out_refs[0].shape[:2]
    copies = [pltpu.make_async_copy(lens_hbm, lens_ref, sem.at[0]), pltpu.make_async_copy(new_hbm.at[pl.ds(0, count)], new_ref, sem.at[1])]
    for j, k in enumerate(ks):
        copies.append(pltpu.make_async_copy(cache_ref.at[pl.ds(0, count), pl.ds((me ^ k) * seq, seq)], out_refs[j], sem.at[2 + j]))
    for c in copies:
        c.start()
    for c in copies:
        c.wait()
    for b in range(count):
        length = lens_ref[b]
        for j, k in enumerate(ks):
            row = length - (me ^ k) * seq

            @pl.when((row >= 0) & (row < seq))
            def _():
                out_refs[j][b, row] = new_ref[b]


def first_split(cache, new, lens, count, ks, parts):
    seq_len, heads, dim = cache.shape[1:]
    seq = seq_len // parts
    return pl.pallas_call(
        functools.partial(first_split_kernel, ks),
        out_shape=[pltpu.VMEM((count, seq, heads, dim), cache.dtype) for _ in ks],
        in_specs=[ANY] * 3,
        out_specs=[pl.BlockSpec(memory_space=pltpu.VMEM)] * len(ks),
        scratch_shapes=[
            pltpu.SMEM(lens.shape, lens.dtype),
            pltpu.VMEM((count,) + new.shape[1:], new.dtype),
            pltpu.SemaphoreType.DMA((2 + len(ks),)),
        ],
        compiler_params=pltpu.CompilerParams(vmem_limit_bytes=MOST_BYTES),
        cost_estimate=pl.CostEstimate(flops=1 << 20, bytes_accessed=1 << 20, transcendentals=0),
    )(lens, new, cache)


def join_kernel(segments, parts, used, *refs):
    srcs, out = refs[:used], refs[-4]
    buf, in_sem, out_sem = refs[-3:]
    me = lax.axis_index("tp")

    for b0, b1, where in segments:
        n = per_step(b1 - b0)

        def load(i, slot):
            return [
                pltpu.make_async_copy(srcs[r].at[pl.ds(off + i * n, n)], buf.at[slot, pl.ds(0, n), :, me ^ k], in_sem.at[slot])
                for k, (r, off) in enumerate(where)
            ]

        def loaded(i, slot):
            return [pltpu.make_async_copy(out.at[pl.ds(b0, n)], buf.at[slot, pl.ds(0, n)], in_sem.at[slot])]

        def store(i, slot):
            return [pltpu.make_async_copy(buf.at[slot, pl.ds(0, n)], out.at[pl.ds(b0 + i * n, n)], out_sem.at[slot])]

        ring_loop((b1 - b0) // n, load, loaded, lambda i, slot: None, store)


def join(pieces, bounds, batch, parts, prev, after, limit):
    keys = list(pieces)
    seq, heads, dim = pieces[keys[0]].shape[1:]
    segments = []
    for b0, b1 in zip(bounds[:-1], bounds[1:]):
        where = []
        for k in range(parts):
            key = next(key for key in keys if key[0] == k and key[1] <= b0 and b1 <= key[2])
            where.append((keys.index(key), b0 - key[1]))
        segments.append((b0, b1, where))
    args = [pieces[key] for key in keys] + ([] if prev is None else [prev]) + list(after)
    moved = 2 * 2 * seq * heads * dim * parts * (bounds[-1] - bounds[0])
    return pl.pallas_call(
        functools.partial(join_kernel, segments, parts, len(keys)),
        out_shape=jax.ShapeDtypeStruct((batch, seq, parts, heads, dim), pieces[keys[0]].dtype),
        in_specs=[ANY] * len(args),
        out_specs=ANY,
        input_output_aliases={} if prev is None else {len(keys): 0},
        scratch_shapes=[
            pltpu.VMEM((RING, max(per_step(b1 - b0) for b0, b1, _ in segments), seq, parts, heads, dim), pieces[keys[0]].dtype),
            pltpu.SemaphoreType.DMA((RING,)),
            pltpu.SemaphoreType.DMA((RING,)),
        ],
        compiler_params=pltpu.CompilerParams(vmem_limit_bytes=limit),
        cost_estimate=pl.CostEstimate(flops=moved * 4, bytes_accessed=moved, transcendentals=0),
    )(*args)


def last_join_kernel(b0, parts, *refs):
    srcs, out, sem = refs[:parts], refs[-2], refs[-1]
    me = lax.axis_index("tp")
    copies = [pltpu.make_async_copy(srcs[k], out.at[pl.ds(b0, srcs[k].shape[0]), :, me ^ k], sem.at[k]) for k in range(parts)]
    for c in copies:
        c.start()
    for c in copies:
        c.wait()


def last_join(pieces, b0, prev):
    parts = len(pieces)
    return pl.pallas_call(
        functools.partial(last_join_kernel, b0, parts),
        out_shape=jax.ShapeDtypeStruct(prev.shape, prev.dtype),
        in_specs=[pl.BlockSpec(memory_space=pltpu.VMEM)] * parts + [ANY],
        out_specs=ANY,
        input_output_aliases={parts: 0},
        scratch_shapes=[pltpu.SemaphoreType.DMA((parts,))],
        compiler_params=pltpu.CompilerParams(vmem_limit_bytes=SMALL_BYTES),
        cost_estimate=pl.CostEstimate(flops=1 << 20, bytes_accessed=1 << 20, transcendentals=0),
    )(*pieces, prev)


def solution(mesh):
    tp = mesh.shape["tp"]

    def local_step(query, k_cache, v_cache, k_new, v_new, lens):
        batch, seq_len, heads, head_dim = k_cache.shape
        seq = seq_len // tp
        group = query.shape[1] // heads

        def send(arr, k):
            return arr if k == 0 else lax.ppermute(arr, "tp", [(i, i ^ k) for i in range(tp)])

        lead = [k for k in (2, 4) if k < tp]
        rest = [k for k in (3, 5, 6, 7, 1, 0) if k < tp]
        order = lead + rest
        c1, c2 = batch // 16, batch // 2 - 2
        v1, v2 = batch - batch // 4, batch - 1
        got = ({}, {})

        def emit(which, groups, outs, after):
            cache, new = ((k_cache, k_new), (v_cache, v_new))[which]
            arrs = split(cache, new, lens, groups, outs, tp, after, MOST_BYTES)
            for key, arr in zip(outs, arrs):
                got[which][key] = send(arr, key[0])
            return [arrs[-1]]

        tok = first_split(k_cache, k_new, lens, c1, lead, tp)
        for k, arr in zip(lead, tok):
            got[0][k, 0, c1] = send(arr, k)
        tok = emit(0, [(c1, c2, lead, per_step(c2 - c1))], [(k, c1, c2) for k in lead], [])
        tok = emit(0, [(c2, batch, order, per_step(batch - c2)), (0, c2, rest, per_step(c2))],
                   [(k, c2, batch) for k in lead] + [(k, 0, batch) for k in rest], tok)
        vb = [0, v1, v2, batch]
        tok = emit(1, [(0, v1, order, per_step(v1))], [(k, 0, v1) for k in order], tok)

        kc, vc, _ = lax.optimization_barrier((k_cache, v_cache, tok))
        slot = lax.broadcasted_iota(jnp.int32, (1, seq_len, 1, 1), 1) == lens[:, None, None, None]
        k_upd = jnp.where(slot, k_new[:, None], kc)
        v_upd = jnp.where(slot, v_new[:, None], vc)
        q_grp = query.reshape(batch, heads, group, head_dim)
        scores = jnp.einsum("bhgd,bthd->bhgt", q_grp, k_upd, preferred_element_type=jnp.float32) * (head_dim ** -0.5)
        valid = lax.broadcasted_iota(jnp.int32, (1, 1, 1, seq_len), 3) <= lens[:, None, None, None]
        probs = jax.nn.softmax(jnp.where(valid, scores, -1e30), axis=-1)
        out = jnp.einsum("bhgt,bthd->bhgd", probs.astype(jnp.bfloat16), v_upd, preferred_element_type=jnp.float32)
        attn = out.reshape(batch, heads * group, head_dim).astype(jnp.bfloat16)

        k_out = join(got[0], [0, c1, c2, batch], batch, tp, None, [attn], MOST_BYTES)
        tok = emit(1, [(v1, v2, order, per_step(v2 - v1))], [(k, v1, v2) for k in order], [k_out])
        emit(1, [(v2, batch, order, 1)], [(k, v2, batch) for k in order], tok)
        v_out, after = None, [k_out]
        for lo, hi in zip(vb[:-2], vb[1:-1]):
            part = {key: arr for key, arr in got[1].items() if key[1] == lo}
            v_out = join(part, [lo, hi], batch, tp, v_out, after, SMALL_BYTES)
            after = []
        v_out = last_join([got[1][k, v2, batch] for k in range(tp)], v2, v_out)
        shape = (batch, seq, tp * heads, head_dim)
        return attn, k_out.reshape(shape), v_out.reshape(shape)

    head_spec = P("dp", "tp")
    entry_spec = P("dp", None, "tp")
    return jax.shard_map(local_step, mesh=mesh, in_specs=(head_spec, entry_spec, entry_spec, head_spec, head_spec, P("dp")), out_specs=(head_spec, P("dp", "tp"), P("dp", "tp")), check_vma=False)
```

```python
import functools

import jax
import jax.numpy as jnp
from jax import lax
from jax.experimental import pallas as pl
from jax.experimental.pallas import tpu as pltpu
from jax.sharding import PartitionSpec as P

RING = 4
VMEM_BYTES = 67043328
MOST_BYTES = VMEM_BYTES - (3 << 20)
SMALL_BYTES = 40 << 20
ANY = pl.BlockSpec(memory_space=pl.ANY)


def ring_loop(count, load, loaded, work, store, ready=()):
    ring = min(RING, count)

    def go(copies):
        for c in copies:
            c.start()

    def end(copies):
        for c in copies:
            c.wait()

    first = count if count == ring else ring - 1
    for i in range(first):
        go(load(i, i))
    end(ready)

    def step(i, carry):
        slot = lax.rem(i, ring)
        end(loaded(i, slot))
        work(i, slot)
        go(store(i, slot))
        if first < count:
            ahead = i + first
            nxt = lax.rem(ahead, ring)

            @pl.when(ahead < count)
            def _():
                @pl.when(i > 0)
                def _():
                    end(store(i - 1, nxt))

                go(load(ahead, nxt))

        return carry

    lax.fori_loop(0, count, step, 0)
    for i in range(count - ring, count):
        end(store(i, i % ring))


def per_step(count):
    return next(n for n in range(8, 0, -1) if count % n == 0)


def split_kernel(groups, outs, lens_hbm, new_hbm, cache_ref, *refs):
    out_refs = refs[-6 - len(outs) : -6]
    buf, lens_ref, new_ref, in_sem, out_sem, small_sem = refs[-6:]
    ready = [
        pltpu.make_async_copy(lens_hbm, lens_ref, small_sem.at[0]),
        pltpu.make_async_copy(new_hbm, new_ref, small_sem.at[1]),
    ]
    for c in ready:
        c.start()
    me = lax.axis_index("tp")
    seq_len = buf.shape[2]
    seq = seq_len // lax.axis_size("tp")

    for b0, b1, ks, n in groups:
        dests = []
        for k in ks:
            i = next(i for i, (ok, lo, hi) in enumerate(outs) if ok == k and lo <= b0 and b1 <= hi)
            dests.append((out_refs[i], b0 - outs[i][1]))

        def load(i, slot):
            rows = pl.ds(b0 + i * n, n)
            if 2 * len(ks) > lax.axis_size("tp"):
                return [pltpu.make_async_copy(cache_ref.at[rows], buf.at[slot, pl.ds(0, n)], in_sem.at[slot, 0])]
            return [
                pltpu.make_async_copy(
                    cache_ref.at[rows, pl.ds((me ^ k) * seq, seq)],
                    buf.at[slot, pl.ds(0, n), pl.ds((me ^ k) * seq, seq)],
                    in_sem.at[slot, j],
                )
                for j, k in enumerate(ks)
            ]

        def store(i, slot):
            return [
                pltpu.make_async_copy(
                    buf.at[slot, pl.ds(0, n), pl.ds((me ^ k) * seq, seq)], ref.at[pl.ds(off + i * n, n)], out_sem.at[slot, j]
                )
                for j, (k, (ref, off)) in enumerate(zip(ks, dests))
            ]

        def work(i, slot):
            for r in range(n):
                b = b0 + i * n + r
                buf[slot, r, lens_ref[b]] = new_ref[b]

        ring_loop((b1 - b0) // n, load, load, work, store, ready)
        ready = []


def split(cache, new, lens, groups, outs, parts, after, limit):
    seq_len, heads, dim = cache.shape[1:]
    seq = seq_len // parts
    moved = 2 * 2 * seq * heads * dim * sum((b1 - b0) * len(ks) for b0, b1, ks, _ in groups)
    return pl.pallas_call(
        functools.partial(split_kernel, groups, outs),
        out_shape=[jax.ShapeDtypeStruct((hi - lo, seq, heads, dim), cache.dtype) for _, lo, hi in outs],
        in_specs=[ANY] * (3 + len(after)),
        out_specs=[ANY] * len(outs),
        scratch_shapes=[
            pltpu.VMEM((RING, max(n for _, _, _, n in groups), seq_len, heads, dim), cache.dtype),
            pltpu.SMEM(lens.shape, lens.dtype),
            pltpu.VMEM(new.shape, new.dtype),
            pltpu.SemaphoreType.DMA((RING, parts)),
            pltpu.SemaphoreType.DMA((RING, parts)),
            pltpu.SemaphoreType.DMA((2,)),
        ],
        compiler_params=pltpu.CompilerParams(vmem_limit_bytes=limit),
        cost_estimate=pl.CostEstimate(flops=moved * 4, bytes_accessed=moved, transcendentals=0),
    )(lens, new, cache, *after)


def first_split_kernel(ks, lens_hbm, new_hbm, cache_ref, *refs):
    out_refs = refs[: len(ks)]
    lens_ref, new_ref, sem = refs[len(ks) :]
    me = lax.axis_index("tp")
    count, seq = out_refs[0].shape[:2]
    copies = []
    for j, k in enumerate(ks):
        copies.append(pltpu.make_async_copy(cache_ref.at[pl.ds(0, count), pl.ds((me ^ k) * seq, seq)], out_refs[j], sem.at[2 + j]))
    copies.append(pltpu.make_async_copy(new_hbm.at[pl.ds(0, count)], new_ref, sem.at[1]))
    copies.insert(0, pltpu.make_async_copy(lens_hbm, lens_ref, sem.at[0]))
    for c in copies:
        c.start()
    for c in copies:
        c.wait()
    for b in range(count):
        length = lens_ref[b]
        for j, k in enumerate(ks):
            row = length - (me ^ k) * seq

            @pl.when((row >= 0) & (row < seq))
            def _():
                out_refs[j][b, row] = new_ref[b]


def first_split(cache, new, lens, count, ks, parts):
    seq_len, heads, dim = cache.shape[1:]
    seq = seq_len // parts
    return pl.pallas_call(
        functools.partial(first_split_kernel, ks),
        out_shape=[pltpu.VMEM((count, seq, heads, dim), cache.dtype) for _ in ks],
        in_specs=[ANY] * 3,
        out_specs=[pl.BlockSpec(memory_space=pltpu.VMEM)] * len(ks),
        scratch_shapes=[
            pltpu.SMEM(lens.shape, lens.dtype),
            pltpu.VMEM((count,) + new.shape[1:], new.dtype),
            pltpu.SemaphoreType.DMA((2 + len(ks),)),
        ],
        compiler_params=pltpu.CompilerParams(vmem_limit_bytes=MOST_BYTES),
        cost_estimate=pl.CostEstimate(flops=1 << 20, bytes_accessed=1 << 20, transcendentals=0),
    )(lens, new, cache)


def join_kernel(segments, parts, used, *refs):
    srcs, out = refs[:used], refs[-4]
    buf, in_sem, out_sem = refs[-3:]
    me = lax.axis_index("tp")

    for b0, b1, where in segments:
        n = per_step(b1 - b0)

        def load(i, slot):
            return [
                pltpu.make_async_copy(srcs[r].at[pl.ds(off + i * n, n)], buf.at[slot, pl.ds(0, n), :, me ^ k], in_sem.at[slot])
                for k, (r, off) in enumerate(where)
            ]

        def loaded(i, slot):
            return [pltpu.make_async_copy(out.at[pl.ds(b0, n)], buf.at[slot, pl.ds(0, n)], in_sem.at[slot])]

        def store(i, slot):
            return [pltpu.make_async_copy(buf.at[slot, pl.ds(0, n)], out.at[pl.ds(b0 + i * n, n)], out_sem.at[slot])]

        ring_loop((b1 - b0) // n, load, loaded, lambda i, slot: None, store)


def join(pieces, bounds, batch, parts, prev, after, limit):
    keys = list(pieces)
    seq, heads, dim = pieces[keys[0]].shape[1:]
    segments = []
    for b0, b1 in zip(bounds[:-1], bounds[1:]):
        where = []
        for k in range(parts):
            key = next(key for key in keys if key[0] == k and key[1] <= b0 and b1 <= key[2])
            where.append((keys.index(key), b0 - key[1]))
        segments.append((b0, b1, where))
    args = [pieces[key] for key in keys] + ([] if prev is None else [prev]) + list(after)
    moved = 2 * 2 * seq * heads * dim * parts * (bounds[-1] - bounds[0])
    return pl.pallas_call(
        functools.partial(join_kernel, segments, parts, len(keys)),
        out_shape=jax.ShapeDtypeStruct((batch, seq, parts, heads, dim), pieces[keys[0]].dtype),
        in_specs=[ANY] * len(args),
        out_specs=ANY,
        input_output_aliases={} if prev is None else {len(keys): 0},
        scratch_shapes=[
            pltpu.VMEM((RING, max(per_step(b1 - b0) for b0, b1, _ in segments), seq, parts, heads, dim), pieces[keys[0]].dtype),
            pltpu.SemaphoreType.DMA((RING,)),
            pltpu.SemaphoreType.DMA((RING,)),
        ],
        compiler_params=pltpu.CompilerParams(vmem_limit_bytes=limit),
        cost_estimate=pl.CostEstimate(flops=moved * 4, bytes_accessed=moved, transcendentals=0),
    )(*args)


def last_join_kernel(b0, parts, *refs):
    srcs, out, sem = refs[:parts], refs[-2], refs[-1]
    me = lax.axis_index("tp")
    copies = [pltpu.make_async_copy(srcs[k], out.at[pl.ds(b0, srcs[k].shape[0]), :, me ^ k], sem.at[k]) for k in range(parts)]
    for c in copies:
        c.start()
    for c in copies:
        c.wait()


def last_join(pieces, b0, prev):
    parts = len(pieces)
    return pl.pallas_call(
        functools.partial(last_join_kernel, b0, parts),
        out_shape=jax.ShapeDtypeStruct(prev.shape, prev.dtype),
        in_specs=[pl.BlockSpec(memory_space=pltpu.VMEM)] * parts + [ANY],
        out_specs=ANY,
        input_output_aliases={parts: 0},
        scratch_shapes=[pltpu.SemaphoreType.DMA((parts,))],
        compiler_params=pltpu.CompilerParams(vmem_limit_bytes=SMALL_BYTES),
        cost_estimate=pl.CostEstimate(flops=1 << 20, bytes_accessed=1 << 20, transcendentals=0),
    )(*pieces, prev)


def solution(mesh):
    tp = mesh.shape["tp"]

    def local_step(query, k_cache, v_cache, k_new, v_new, lens):
        batch, seq_len, heads, head_dim = k_cache.shape
        seq = seq_len // tp
        group = query.shape[1] // heads

        def send(arr, k):
            return arr if k == 0 else lax.ppermute(arr, "tp", [(i, i ^ k) for i in range(tp)])

        lead = [k for k in (2, 4) if k < tp]
        rest = [k for k in (3, 5, 6, 7, 1, 0) if k < tp]
        order = lead + rest
        c1, c2 = batch // 16, batch // 2 - 2
        v1, v2 = batch - batch // 4, batch - 1
        got = ({}, {})

        def emit(which, groups, outs, after):
            cache, new = ((k_cache, k_new), (v_cache, v_new))[which]
            arrs = split(cache, new, lens, groups, outs, tp, after, MOST_BYTES)
            for key, arr in zip(outs, arrs):
                got[which][key] = send(arr, key[0])
            return [arrs[-1]]

        tok = first_split(k_cache, k_new, lens, c1, lead, tp)
        for k, arr in zip(lead, tok):
            got[0][k, 0, c1] = send(arr, k)
        tok = emit(0, [(c1, c2, lead, per_step(c2 - c1))], [(k, c1, c2) for k in lead], [])
        tok = emit(0, [(c2, batch, order, per_step(batch - c2)), (0, c2, rest, per_step(c2))],
                   [(k, c2, batch) for k in lead] + [(k, 0, batch) for k in rest], tok)
        vb = [0, v1, v2, batch]
        tok = emit(1, [(0, v1, order, per_step(v1))], [(k, 0, v1) for k in order], tok)

        kc, vc, _ = lax.optimization_barrier((k_cache, v_cache, tok))
        slot = lax.broadcasted_iota(jnp.int32, (1, seq_len, 1, 1), 1) == lens[:, None, None, None]
        k_upd = jnp.where(slot, k_new[:, None], kc)
        v_upd = jnp.where(slot, v_new[:, None], vc)
        q_grp = query.reshape(batch, heads, group, head_dim)
        scores = jnp.einsum("bhgd,bthd->bhgt", q_grp, k_upd, preferred_element_type=jnp.float32) * (head_dim ** -0.5)
        valid = lax.broadcasted_iota(jnp.int32, (1, 1, 1, seq_len), 3) <= lens[:, None, None, None]
        probs = jax.nn.softmax(jnp.where(valid, scores, -1e30), axis=-1)
        out = jnp.einsum("bhgt,bthd->bhgd", probs.astype(jnp.bfloat16), v_upd, preferred_element_type=jnp.float32)
        attn = out.reshape(batch, heads * group, head_dim).astype(jnp.bfloat16)

        k_out = join(got[0], [0, c1, c2, batch], batch, tp, None, [attn], MOST_BYTES)
        tok = emit(1, [(v1, v2, order, per_step(v2 - v1))], [(k, v1, v2) for k in order], [k_out])
        emit(1, [(v2, batch, order, 1)], [(k, v2, batch) for k in order], tok)
        v_out, after = None, [k_out]
        for lo, hi in zip(vb[:-2], vb[1:-1]):
            part = {key: arr for key, arr in got[1].items() if key[1] == lo}
            v_out = join(part, [lo, hi], batch, tp, v_out, after, SMALL_BYTES)
            after = []
        v_out = last_join([got[1][k, v2, batch] for k in range(tp)], v2, v_out)
        shape = (batch, seq, tp * heads, head_dim)
        return attn, k_out.reshape(shape), v_out.reshape(shape)

    head_spec = P("dp", "tp")
    entry_spec = P("dp", None, "tp")
    return jax.shard_map(local_step, mesh=mesh, in_specs=(head_spec, entry_spec, entry_spec, head_spec, head_spec, P("dp")), out_specs=(head_spec, P("dp", "tp"), P("dp", "tp")), check_vma=False)
```
